32 devices in a mesh: groups: 2 (over y), seq: 4 (over z), tensor: 2 (over x), cfg: 2 (over core).
Axes of the slice: x: 2, y: 2, z: 4, core: 2. Of those that a mesh axis runs over, the one named last changes fastest.
Arguments:
- latent: bfloat16 [2048, 3072], P(('groups', 'seq')), parts along dimension 0, may hold values from -6 to 6
- positions: int32 [3, 2048], P(None, ('groups', 'seq')), parts along dimension 1, may hold values from 0 to 79, as said below
- text_kv: bfloat16 [2, 2, 128, 3072], P('cfg', None, ('groups', 'seq'), 'tensor'), parts along dimension 2, may hold values from -6 to 6
- text_len: int32 [4], P(('groups', 'cfg')), parts along dimension 0, may hold values from 1 to 64
- modulation: float32 [3, 4, 3072], P(None, 'groups'), parts along dimension 1, may hold values from -3 to 3
- w_qkv: bfloat16 [3, 3072, 3072], P(None, 'cfg', 'tensor'), may hold values from -0.109375 to 0.109375
- norm_gains: float32 [2, 128], replicated, may hold values from 0.5 to 2.5
- w_out: bfloat16 [3072, 3072], P('tensor', 'cfg'), may hold values from -0.109375 to 0.109375
- guidance: float32 [2], P('groups'), parts along dimension 0, may hold values from 3 to 8
Outputs:
- guided: bfloat16 [2048, 3072], P(('groups', 'seq', 'tensor'), 'cfg'), parts along dimension 0
The draws below stay inside these ranges and needn't reach their ends.
There are 2 independent parts, one for each index of `groups`. The reference program is written for one: setup_inputs(seed, part) draws one part's arguments, and reference() takes and returns one part's arrays. A program takes and returns all parts, laid end to end along the dimension named above; an argument that names none is the same for every part. Nothing has to cross between parts.
Inputs may be any that keep to these rules, and one draw needn't show every extreme that they name: `positions`: frame indices are below 33, height indices below 45, width indices below 80. `text_len`: text rows at or beyond the count are ignored.
All inputs are finite; a program needn't handle non-finite values.
Results may differ from the reference program's by a relative error of at most 0.018.
Values may be sent and summed in bfloat16 or wider, within the bound.
A program may use at most 128 MiB of HBM per device.

```python
import math
import jax
import jax.numpy as jnp
from jax import lax

D = 3072
HEADS = 24
HEAD_DIM = 128
TOKENS = 1024
TEXT = 64


def draw_positions(key, part):
    keys = jax.random.split(jax.random.fold_in(key, 11), 3)
    frame = jax.random.randint(keys[0], (TOKENS,), 0, 33)
    height = jax.random.randint(keys[1], (TOKENS,), 0, 45)
    across = jax.random.randint(keys[2], (TOKENS,), 0, 80)
    return jnp.stack([frame, height, across]).astype(jnp.int32)


def level_of(stream_key, extent, cuts, smallest, largest):
    level, own = 1.0, jax.random.fold_in(stream_key, 6)
    for dim, shards_of in cuts:
        heights = jnp.exp(jax.random.uniform(jax.random.fold_in(own, dim), (shards_of,), jnp.float32, smallest / len(cuts), largest / len(cuts)))
        level = level * jnp.repeat(heights, extent[dim] // shards_of).reshape([-1 if axis == dim else 1 for axis in range(len(extent))])
    return level


def normal_values(stream_key, extent, scale, bound, cuts=(), kind=jnp.bfloat16):
    entries = jax.random.normal(stream_key, extent, jnp.float32) * scale
    if len(cuts) > 0:
        entries = level_of(stream_key, extent, cuts, -0.22, 0.18) * entries
    return jnp.clip(entries, min=-bound, max=bound).astype(kind)


def setup_inputs(seed: int = 0, part: int = 0) -> dict:
    splits = jax.random.split(jax.random.key(seed), 10)
    own_keys = jax.random.split(jax.random.fold_in(splits[9], part), 10)
    return {
        "latent": normal_values(own_keys[0], (TOKENS, D), 1.0, 6.0, ((0, 4),)),
        "positions": draw_positions(jax.random.fold_in(jax.random.fold_in(splits[9], part), 71), part),
        "text_kv": normal_values(own_keys[2], (2, 2, TEXT, D), 1.0, 6.0, ((0, 2), (2, 4), (3, 2))),
        "text_len": jax.random.randint(own_keys[3], (2,), 1, TEXT + 1).astype(jnp.int32),
        "modulation": normal_values(own_keys[4], (3, 2, D), 0.5, 3.0, (), jnp.float32),
        "w_qkv": normal_values(splits[5], (3, D, D), D ** -0.5, 0.109375, ((1, 2), (2, 2))),
        "norm_gains": jnp.clip(jnp.exp(jax.random.uniform(splits[6], (2, HEAD_DIM), jnp.float32, math.log(0.5), math.log(2.5))), 0.5, 2.5),
        "w_out": normal_values(splits[7], (D, D), D ** -0.5, 0.109375, ((0, 2), (1, 2))),
        "guidance": jnp.clip(jax.random.uniform(own_keys[8], (1,), jnp.float32, 3.0, 8.0), 3.0, 8.0),
    }


def head_norm(heads_in, gain):
    return heads_in * lax.rsqrt(lax.optimization_barrier(jnp.mean(heads_in * heads_in, axis=-1, keepdims=True)) + 1e-06) * gain

def rotary(heads_in, positions):
    head_size = heads_in.shape[-1]
    blocks = (head_size // 8, 7 * head_size // 16, 7 * head_size // 16)
    pieces = []
    offset = 0
    for axis_id in range(3):
        width = blocks[axis_id]
        half = width // 2
        freq = 256.0 ** (-jnp.arange(half, dtype=jnp.float32) / half)
        angle = positions[axis_id].astype(jnp.float32)[:, None] * freq[None, :]
        cosine = jnp.cos(angle)[:, None, :]
        sine = jnp.sin(angle)[:, None, :]
        first = heads_in[..., offset:offset + half]
        second = heads_in[..., offset + half:offset + width]
        pieces.append(first * cosine - second * sine)
        pieces.append(second * cosine + first * sine)
        offset = offset + width
    return jnp.concatenate(pieces, axis=-1)

def reference(latent, positions, text_kv, text_len, modulation, w_qkv, norm_gains, w_out, guidance):
    rows = latent.shape[0]
    xfloat = latent.astype(jnp.float32)
    center = xfloat - lax.optimization_barrier(jnp.mean(xfloat, axis=-1, keepdims=True))
    normed = center * lax.rsqrt(lax.optimization_barrier(jnp.mean(center * center, axis=-1, keepdims=True)) + 1e-06)
    scale = HEAD_DIM ** (-0.5)
    outputs = []
    for branch in range(2):
        modulated = (normed * (1.0 + modulation[1, branch]) + modulation[0, branch]).astype(jnp.bfloat16)
        projected = [jnp.dot(modulated, w_qkv[j], preferred_element_type=jnp.float32) for j in range(3)]
        queries = rotary(head_norm(projected[0].reshape(rows, HEADS, HEAD_DIM), norm_gains[0]), positions).astype(jnp.bfloat16)
        keys = rotary(head_norm(projected[1].reshape(rows, HEADS, HEAD_DIM), norm_gains[1]), positions).astype(jnp.bfloat16)
        value_rows = projected[2].astype(jnp.bfloat16).reshape(rows, HEADS, HEAD_DIM)
        prompt_keys = head_norm(text_kv[branch, 0].astype(jnp.float32).reshape(TEXT, HEADS, HEAD_DIM), norm_gains[1]).astype(jnp.bfloat16)
        all_keys = jnp.concatenate([keys, prompt_keys], axis=0)
        all_values = jnp.concatenate([value_rows, text_kv[branch, 1].reshape(TEXT, HEADS, HEAD_DIM)], axis=0)
        valid = jnp.concatenate([jnp.ones((rows,), bool), jnp.arange(TEXT, dtype=jnp.int32) < text_len[branch]])

        def one_head(operands):
            query_head, key_head, value_head = operands
            scores = jnp.dot(query_head, key_head.T, preferred_element_type=jnp.float32) * scale
            expo = jnp.where(valid[None, :], jnp.exp(scores), 0.0)
            total = lax.optimization_barrier(jnp.sum(expo, axis=-1, keepdims=True))
            mixed = jnp.dot(expo.astype(jnp.bfloat16), value_head, preferred_element_type=jnp.float32)
            return mixed / total
        attended = lax.map(one_head, (queries.transpose(1, 0, 2), all_keys.transpose(1, 0, 2), all_values.transpose(1, 0, 2)))
        attended = attended.transpose(1, 0, 2).reshape(rows, HEADS * HEAD_DIM).astype(jnp.bfloat16)
        branch_out = (modulation[2, branch] * jnp.dot(attended, w_out, preferred_element_type=jnp.float32)).astype(jnp.bfloat16)
        outputs.append(lax.optimization_barrier(branch_out).astype(jnp.float32))
    return (outputs[1] + guidance[0] * (outputs[0] - outputs[1])).astype(jnp.bfloat16)
```

```python
import functools

import jax
import jax.numpy as jnp
import numpy as np
from jax import lax
from jax.experimental import pallas as pl
from jax.experimental.pallas import tpu as pltpu
from jax.sharding import PartitionSpec as P

HEAD_DIM = 128
MESH = pl.DeviceIdType.MESH
F32 = jnp.float32
BF16 = jnp.bfloat16


def rotary_rows(head_size):
    rows = np.zeros((8, head_size), np.float32)
    axes = np.zeros((head_size,), np.int32)
    blocks = (head_size // 8, 7 * head_size // 16, 7 * head_size // 16)
    halves = []
    offset = 0
    for axis_id, width in enumerate(blocks):
        half = width // 2
        if half not in halves:
            halves.append(half)
        which = halves.index(half)
        freq = (256.0 ** (-np.arange(half, dtype=np.float64) / half)).astype(np.float32)
        rows[0, offset : offset + half] = freq
        rows[0, offset + half : offset + width] = freq
        rows[1 + 2 * which, offset : offset + half] = -1.0
        rows[2 + 2 * which, offset + half : offset + width] = 1.0
        axes[offset : offset + width] = axis_id
        offset += width
    shifts = []
    for half in halves:
        shifts += [head_size - half, half]
    return rows, axes, tuple(shifts)


ROT_ROWS, ROT_AXES, ROT_SHIFTS = rotary_rows(HEAD_DIM)


def kernel(
    seq_n,
    ten_n,
    latent,
    pos_lanes,
    text_kv,
    lens_in,
    modulation,
    w_qkv,
    gains,
    w_out,
    mix,
    rot,
    out,
    lat,
    pos,
    txt,
    lens,
    wfull,
    wout,
    mod,
    tab,
    qbuf,
    kbuf,
    vbuf,
    acc,
    lsum,
    attf,
    part,
    got,
    send_a,
    recv_a,
    send_b,
    recv_b,
    send_c,
    recv_c,
    send_p,
    recv_p,
    send_t,
    recv_t,
    send_w,
    recv_w,
    send_l,
    recv_l,
    send_o,
    recv_o,
    send_r,
    recv_r,
    loc,
):
    x = lax.axis_index("tensor")
    c = lax.axis_index("cfg")
    z = lax.axis_index("seq")
    other = 1 - c
    rows, width = latent.shape
    half = w_qkv.shape[1]
    mine = wfull.shape[2]
    heads = mine // HEAD_DIM
    half_rows = rows // 2
    piece = half_rows // ten_n
    out_rows = rows // ten_n
    out_cols = w_out.shape[1]
    scale = HEAD_DIM ** (-0.5)
    tile = 256 if mine % 256 == 0 else 128
    per_tile = tile // HEAD_DIM
    shorter = jnp.minimum(z, seq_n - 1 - z)
    long_sign = jnp.where(2 * z < seq_n - 1, 1, -1)

    def order(i):
        near = i <= 2 * shorter
        dist = jnp.where(near, (i + 1) // 2, i - shorter)
        sign = jnp.where(near, 2 * (i % 2) - 1, long_sign)
        return jnp.where(i == 0, z, z + dist * sign)

    def remote(src, dst, send, recv, **to):
        return pltpu.make_async_remote_copy(
            src_ref=src, dst_ref=dst, send_sem=send, recv_sem=recv, device_id=to, device_id_type=MESH
        )

    def aligned(value, unit):
        return pl.multiple_of(value * unit, unit)

    cols_of = lambda core: pl.ds(aligned(core, mine), mine)
    w_copy = [
        remote(
            w_qkv.at[j, :, cols_of(other)],
            wfull.at[j, pl.ds(aligned(c, half), half), :],
            send_w.at[j],
            recv_w.at[j],
            cfg=other,
        )
        for j in range(3)
    ]
    w_local = [
        pltpu.make_async_copy(
            w_qkv.at[j, :, cols_of(c)], wfull.at[j, pl.ds(aligned(c, half), half), :], loc.at[j]
        )
        for j in range(3)
    ]
    lat_local = pltpu.make_async_copy(latent, lat.at[z], loc.at[3])
    pos_local = pltpu.make_async_copy(pos_lanes, pos.at[z], loc.at[4])
    txt_local = pltpu.make_async_copy(text_kv.at[0, :, :, cols_of(c)], txt.at[c, z], loc.at[5])
    len_local = pltpu.make_async_copy(lens_in, lens.at[c], loc.at[6])
    out_local = pltpu.make_async_copy(w_out, wout, loc.at[7])
    my_piece = pl.ds(pl.multiple_of((c * ten_n + x) * piece, piece), piece)

    def copy_a(i):
        return remote(
            latent.at[my_piece], lat.at[z, my_piece], send_a.at[i], recv_a.at[z], seq=order(i)
        )

    def arrived_a(o):
        return remote(
            latent.at[my_piece], lat.at[o, my_piece], send_a.at[0], recv_a.at[o], seq=order(1)
        )

    def copy_b(o, t):
        to = (x + t) % ten_n
        return remote(
            lat.at[o, my_piece], lat.at[o, my_piece], send_b.at[o, t], recv_b.at[o, t], tensor=to
        )

    def arrived_b(o, t):
        source = (x + ten_n - t) % ten_n
        landed = pl.ds(pl.multiple_of((c * ten_n + source) * piece, piece), piece)
        return remote(
            lat.at[o, landed], lat.at[o, landed], send_b.at[o, t], recv_b.at[o, t], tensor=source
        )

    def copy_c(o, core):
        at = pl.ds(aligned(core, half_rows), half_rows)
        return remote(lat.at[o, at], lat.at[o, at], send_c.at[o], recv_c.at[o], cfg=other)

    def copy_p(i):
        return remote(pos_lanes, pos.at[z], send_p.at[i], recv_p.at[z], seq=order(i))

    def arrived_p(o):
        return remote(pos_lanes, pos.at[o], send_p.at[0], recv_p.at[o], seq=order(1))

    def copy_t(i, core):
        return remote(
            text_kv.at[0, :, :, cols_of(core)],
            txt.at[c, z],
            send_t.at[core, i],
            recv_t.at[c, z],
            seq=order(i),
            cfg=core,
        )

    def copy_t_mirror():
        return remote(
            text_kv.at[0, :, :, cols_of(other)],
            txt.at[c, z],
            send_t.at[other, 0],
            recv_t.at[c, z],
            cfg=other,
        )

    def arrived_t(core, o):
        return remote(
            text_kv.at[0, :, :, cols_of(c)], txt.at[core, o], send_t.at[c, 0], recv_t.at[core, o], cfg=other
        )

    def copy_l(core):
        return remote(lens_in, lens.at[core], send_l.at[0], recv_l.at[0], cfg=other)

    for j in range(3):
        w_local[j].start()
    lat_local.start()
    pos_local.start()
    txt_local.start()
    len_local.start()
    out_local.start()

    barrier = pltpu.get_barrier_semaphore()
    pl.semaphore_signal(barrier, inc=1, device_id={"cfg": other}, device_id_type=MESH)
    for t in range(1, ten_n):
        pl.semaphore_signal(
            barrier, inc=1, device_id={"tensor": (x + t) % ten_n}, device_id_type=MESH
        )
    for s in range(1, seq_n):
        for k in range(2):
            pl.semaphore_signal(
                barrier,
                inc=1,
                device_id={"seq": (z + s) % seq_n, "cfg": (c + k) % 2},
                device_id_type=MESH,
            )
    pl.semaphore_wait(barrier, 1 + (ten_n - 1) + 2 * (seq_n - 1))

    for j in range(3):
        w_copy[j].start()

    @pl.loop(1, seq_n)
    def _(i):
        copy_p(i).start()
        copy_a(i).start()

    copy_l(c).start()
    copy_t_mirror().start()

    @pl.loop(1, seq_n)
    def _(i):
        copy_t(i, 0).start()
        copy_t(i, 1).start()

    acc[...] = jnp.zeros_like(acc)
    lsum[...] = jnp.zeros_like(lsum)
    lat_local.wait()
    pos_local.wait()

    def pump_a(i):
        o = order(i)
        arrived_a(o).wait_recv()
        for t in range(1, ten_n):
            copy_b(o, t).start()

    def pump_b(i):
        o = order(i)
        for t in range(1, ten_n):
            arrived_b(o, t).wait_recv()
        copy_c(o, c).start()

    def normed_head(value, gain):
        return (
            value * lax.rsqrt(jnp.mean(value * value, axis=-1, keepdims=True) + 1e-06) * gain
        )

    def turned(value):
        total = value * tab[0]
        for k, shift in enumerate(ROT_SHIFTS):
            total = total + pltpu.roll(value, shift, 1) * tab[1 + k]
        return total

    def project(j, t):
        at = pl.ds(pl.multiple_of(t * tile, tile), tile)
        return jnp.dot(mod[...], wfull[j, :, at], preferred_element_type=F32)

    def head_tiles(j, gain_row, dest):
        @pl.loop(0, mine // tile)
        def _(t):
            y = project(j, t)
            gain = gains[gain_row : gain_row + 1, :]
            for hh in range(per_tile):
                for b in range(2):
                    part_in = y[b * rows : (b + 1) * rows, hh * HEAD_DIM : (hh + 1) * HEAD_DIM]
                    dest[b * heads + t * per_tile + hh] = turned(normed_head(part_in, gain)).astype(
                        BF16
                    )

    def value_tiles():
        @pl.loop(0, mine // tile)
        def _(t):
            y = project(2, t).astype(BF16)
            for hh in range(per_tile):
                for b in range(2):
                    vbuf[b * heads + t * per_tile + hh] = y[
                        b * rows : (b + 1) * rows, hh * HEAD_DIM : (hh + 1) * HEAD_DIM
                    ]

    strip = 16

    @pl.loop(0, seq_n)
    def _(i):
        o = order(i)

        @pl.when(i > 0)
        def _():
            arrived_p(o).wait_recv()
            copy_c(o, other).wait_recv()

        angle = pos[o].astype(F32) * rot[0:1, :]
        sine = jnp.sin(angle)
        tab[0] = jnp.cos(angle)
        for k in range(len(ROT_SHIFTS)):
            tab[1 + k] = sine * rot[1 + k : 2 + k, :]

        @pl.loop(0, rows // strip)
        def _(r):
            at = pl.ds(pl.multiple_of(r * strip, strip), strip)
            value = lat[o, at, :].astype(F32)
            center = value - jnp.mean(value, axis=-1, keepdims=True)
            normed = center * lax.rsqrt(jnp.mean(center * center, axis=-1, keepdims=True) + 1e-06)
            for b in range(2):
                mod[pl.ds(pl.multiple_of(b * rows + r * strip, strip), strip), :] = (
                    normed * (1.0 + modulation[1, b : b + 1, :]) + modulation[0, b : b + 1, :]
                ).astype(BF16)

        @pl.when(i == 0)
        def _():
            w_local[0].wait()
            w_copy[0].wait_recv()
            head_tiles(0, 0, qbuf)
            w_local[1].wait()
            w_copy[1].wait_recv()
            if seq_n > 1:
                pump_a(1)

        head_tiles(1, 1, kbuf)

        @pl.when(i == 0)
        def _():
            w_local[2].wait()
            w_copy[2].wait_recv()

        value_tiles()

        @pl.when(i + 2 < seq_n)
        def _():
            pump_a(i + 2)

        @pl.when(i + 1 < seq_n)
        def _():
            pump_b(i + 1)

        @pl.loop(0, 2 * heads)
        def _(h):
            scores = lax.dot_general(
                qbuf[h], kbuf[h], (((1,), (1,)), ((), ())), preferred_element_type=F32
            )
            expo = jnp.exp(scores * scale)
            folded = expo[:, :HEAD_DIM]
            for k in range(1, rows // HEAD_DIM):
                folded = folded + expo[:, k * HEAD_DIM : (k + 1) * HEAD_DIM]
            lsum[h] += folded
            acc[h] += jnp.dot(expo.astype(BF16), vbuf[h], preferred_element_type=F32)

    txt_local.wait()
    len_local.wait()
    copy_l(other).wait_recv()
    arrived_t(other, z).wait_recv()

    @pl.loop(1, seq_n)
    def _(i):
        arrived_t(0, order(i)).wait_recv()
        arrived_t(1, order(i)).wait_recv()

    text_rows = txt.shape[3]
    count = seq_n * text_rows
    for b in range(2):
        valid = lax.broadcasted_iota(jnp.int32, (1, count), 1).astype(F32) < lens[b, 0:1, :]

        @pl.loop(0, heads)
        def _(h):
            at = pl.ds(pl.multiple_of(h * HEAD_DIM, HEAD_DIM), HEAD_DIM)
            raw = txt[b, :, 0, :, at].reshape(count, HEAD_DIM).astype(F32)
            keys = normed_head(raw, gains[1:2, :]).astype(BF16)
            values = txt[b, :, 1, :, at].reshape(count, HEAD_DIM)
            n = b * heads + h
            scores = lax.dot_general(
                qbuf[n], keys, (((1,), (1,)), ((), ())), preferred_element_type=F32
            )
            expo = jnp.where(valid, jnp.exp(scores * scale), 0.0)
            total = jnp.sum(lsum[n], axis=-1, keepdims=True) + jnp.sum(
                expo, axis=-1, keepdims=True
            )
            mixed = acc[n] + jnp.dot(expo.astype(BF16), values, preferred_element_type=F32)
            attf[c, b, :, at] = (mixed / total).astype(BF16)

    def copy_o(core):
        return remote(attf.at[core], attf.at[core], send_o.at[0], recv_o.at[0], cfg=other)

    copy_o(c).start()
    out_local.wait()
    copy_o(other).wait_recv()

    def copy_r(t):
        return remote(part.at[t], got.at[t], send_r.at[t], recv_r.at[t], tensor=(x + t) % ten_n)

    out_tile = 256 if out_cols % 256 == 0 else 128

    def out_block(t, at):
        to = (x + t) % ten_n
        here = pl.ds(pl.multiple_of(to * out_rows, out_rows), out_rows)
        total = None
        for b in range(2):
            y = jnp.dot(attf[0, b, here, :], wout[0:mine, at], preferred_element_type=F32)
            y = y + jnp.dot(
                attf[1, b, here, :], wout[mine : 2 * mine, at], preferred_element_type=F32
            )
            y = y * mix[b : b + 1, at]
            total = y if total is None else total + y
        return total

    for t in range(1, ten_n):

        @pl.loop(0, out_cols // out_tile)
        def _(k):
            at = pl.ds(pl.multiple_of(k * out_tile, out_tile), out_tile)
            part[t, :, at] = out_block(t, at).astype(BF16)

        copy_r(t).start()


    @pl.loop(0, out_cols // out_tile)
    def _(k):
        at = pl.ds(pl.multiple_of(k * out_tile, out_tile), out_tile)
        part[0, :, at] = out_block(0, at).astype(BF16)

    for t in range(1, ten_n):
        copy_r(t).wait_recv()
    total = part[0].astype(F32)
    for t in range(1, ten_n):
        total = total + got[t].astype(F32)
    out[...] = total.astype(BF16)

    for j in range(3):
        w_copy[j].wait_send()
    copy_l(c).wait_send()
    copy_t_mirror().wait_send()
    copy_o(c).wait_send()
    for t in range(1, ten_n):
        copy_r(t).wait_send()

    @pl.loop(1, seq_n)
    def _(i):
        copy_p(i).wait_send()
        copy_a(i).wait_send()
        copy_t(i, 0).wait_send()
        copy_t(i, 1).wait_send()
        o = order(i)
        for t in range(1, ten_n):
            copy_b(o, t).wait_send()
        copy_c(o, c).wait_send()


def local(
    seq_n, ten_n, latent, positions, text_kv, text_len, modulation, w_qkv, norm_gains, w_out, guidance
):
    rows, width = latent.shape
    mine = w_qkv.shape[2] // 2
    heads = mine // HEAD_DIM
    text_dev = text_kv.shape[2]
    out_rows = rows // ten_n
    out_cols = w_out.shape[1]
    core = lax.axis_index("cfg")
    axes = jnp.asarray(ROT_AXES)[None, :]
    place = positions.astype(BF16)[:, :, None]
    pos_lanes = jnp.where(axes == 0, place[0], jnp.where(axes == 1, place[1], place[2]))
    lens = jnp.broadcast_to(text_len.astype(F32)[None, :], (8, seq_n * text_dev))
    gate = lax.dynamic_slice_in_dim(modulation[2], core * out_cols, out_cols, 1)
    strength = guidance[0]
    mix = gate * jnp.stack([strength, 1.0 - strength])[:, None]
    any_space = pl.BlockSpec(memory_space=pl.ANY)
    vmem = pl.BlockSpec(memory_space=pltpu.VMEM)
    dma = pltpu.SemaphoreType.DMA
    return pl.pallas_call(
        functools.partial(kernel, seq_n, ten_n),
        out_shape=jax.ShapeDtypeStruct((out_rows, out_cols), BF16),
        in_specs=[
            any_space,
            any_space,
            any_space,
            any_space,
            vmem,
            any_space,
            vmem,
            any_space,
            vmem,
            vmem,
        ],
        out_specs=vmem,
        scratch_shapes=[
            pltpu.VMEM((seq_n, rows, width), BF16),
            pltpu.VMEM((seq_n, rows, HEAD_DIM), BF16),
            pltpu.VMEM((2, seq_n, 2, text_dev, mine), BF16),
            pltpu.VMEM((2, 8, seq_n * text_dev), F32),
            pltpu.VMEM((3, width, mine), BF16),
            pltpu.VMEM(w_out.shape, BF16),
            pltpu.VMEM((2 * rows, width), BF16),
            pltpu.VMEM((1 + len(ROT_SHIFTS), rows, HEAD_DIM), F32),
            pltpu.VMEM((2 * heads, rows, HEAD_DIM), BF16),
            pltpu.VMEM((2 * heads, rows, HEAD_DIM), BF16),
            pltpu.VMEM((2 * heads, rows, HEAD_DIM), BF16),
            pltpu.VMEM((2 * heads, rows, HEAD_DIM), F32),
            pltpu.VMEM((2 * heads, rows, HEAD_DIM), F32),
            pltpu.VMEM((2, 2, rows, mine), BF16),
            pltpu.VMEM((ten_n, out_rows, out_cols), BF16),
            pltpu.VMEM((ten_n, out_rows, out_cols), BF16),
            dma((seq_n,)),
            dma((seq_n,)),
            dma((seq_n, ten_n)),
            dma((seq_n, ten_n)),
            dma((seq_n,)),
            dma((seq_n,)),
            dma((seq_n,)),
            dma((seq_n,)),
            dma((2, seq_n)),
            dma((2, seq_n)),
            dma((3,)),
            dma((3,)),
            dma((1,)),
            dma((1,)),
            dma((1,)),
            dma((1,)),
            dma((ten_n,)),
            dma((ten_n,)),
            dma((8,)),
        ],
        compiler_params=pltpu.CompilerParams(
            collective_id=0, has_side_effects=True, vmem_limit_bytes=64 * 1024 * 1024 - 65536
        ),
    )(
        latent,
        pos_lanes,
        text_kv,
        lens,
        modulation,
        w_qkv,
        norm_gains,
        w_out,
        mix,
        jnp.asarray(ROT_ROWS),
    )


def solution(mesh):
    placed = (
        P(("groups", "seq"), None),
        P(None, ("groups", "seq")),
        P("cfg", None, ("groups", "seq"), "tensor"),
        P(("groups", "cfg")),
        P(None, "groups", None),
        P(None, "cfg", "tensor"),
        P(),
        P("tensor", "cfg"),
        P("groups"),
    )
    return jax.shard_map(
        functools.partial(local, mesh.shape["seq"], mesh.shape["tensor"]),
        mesh=mesh,
        in_specs=placed,
        out_specs=P(("groups", "seq", "tensor"), "cfg"),
        check_vma=False,
    )
```

```python
import functools

import jax
import jax.numpy as jnp
import numpy as np
from jax import lax
from jax.experimental import pallas as pl
from jax.experimental.pallas import tpu as pltpu
from jax.sharding import PartitionSpec as P

HEAD_DIM = 128
MESH = pl.DeviceIdType.MESH
U_TILE = True
U_MOD = 8
U_ATT = 4
U_TEXT = 2
F32 = jnp.float32
BF16 = jnp.bfloat16


def rotary_rows(head_size):
    rows = np.zeros((8, head_size), np.float32)
    axes = np.zeros((head_size,), np.int32)
    blocks = (head_size // 8, 7 * head_size // 16, 7 * head_size // 16)
    halves = []
    offset = 0
    for axis_id, width in enumerate(blocks):
        half = width // 2
        if half not in halves:
            halves.append(half)
        which = halves.index(half)
        freq = (256.0 ** (-np.arange(half, dtype=np.float64) / half)).astype(np.float32)
        rows[0, offset : offset + half] = freq
        rows[0, offset + half : offset + width] = freq
        rows[1 + 2 * which, offset : offset + half] = -1.0
        rows[2 + 2 * which, offset + half : offset + width] = 1.0
        axes[offset : offset + width] = axis_id
        offset += width
    shifts = []
    for half in halves:
        shifts += [head_size - half, half]
    return rows, axes, tuple(shifts)


ROT_ROWS, ROT_AXES, ROT_SHIFTS = rotary_rows(HEAD_DIM)
ROT_PICK = (np.arange(16)[:, None] == ROT_AXES[None, :]).astype(np.float32)


def kernel(
    seq_n,
    ten_n,
    latent,
    pos_in,
    text_kv,
    lens_in,
    modulation,
    w_qkv,
    gains,
    w_out,
    guide,
    rot,
    pick,
    out,
    lat,
    pos,
    txt,
    lens,
    wfull,
    wout,
    mod,
    tab,
    qbuf,
    kbuf,
    vbuf,
    acc,
    lsum,
    attf,
    part,
    got,
    send_a,
    recv_a,
    send_b,
    recv_b,
    send_c,
    recv_c,
    send_p,
    recv_p,
    send_t,
    recv_t,
    send_w,
    recv_w,
    send_l,
    recv_l,
    send_o,
    recv_o,
    send_r,
    recv_r,
    loc,
):
    x = lax.axis_index("tensor")
    c = lax.axis_index("cfg")
    z = lax.axis_index("seq")
    other = 1 - c
    rows, width = latent.shape
    half = w_qkv.shape[1]
    mine = wfull.shape[2]
    heads = mine // HEAD_DIM
    half_rows = rows // 2
    piece = half_rows // ten_n
    out_rows = rows // ten_n
    out_cols = w_out.shape[1]
    scale = HEAD_DIM ** (-0.5)
    tile = 256 if mine % 256 == 0 else 128
    per_tile = tile // HEAD_DIM
    shorter = jnp.minimum(z, seq_n - 1 - z)
    long_sign = jnp.where(2 * z < seq_n - 1, 1, -1)

    def order(i):
        near = i <= 2 * shorter
        dist = jnp.where(near, (i + 1) // 2, i - shorter)
        sign = jnp.where(near, 2 * (i % 2) - 1, long_sign)
        return jnp.where(i == 0, z, z + dist * sign)

    def remote(src, dst, send, recv, **to):
        return pltpu.make_async_remote_copy(
            src_ref=src, dst_ref=dst, send_sem=send, recv_sem=recv, device_id=to, device_id_type=MESH
        )

    def aligned(value, unit):
        return pl.multiple_of(value * unit, unit)

    cols_of = lambda core: pl.ds(aligned(core, mine), mine)
    w_copy = [
        remote(
            w_qkv.at[j, :, cols_of(other)],
            wfull.at[j, pl.ds(aligned(c, half), half), :],
            send_w.at[j],
            recv_w.at[j],
            cfg=other,
        )
        for j in range(3)
    ]
    w_local = [
        pltpu.make_async_copy(
            w_qkv.at[j, :, cols_of(c)], wfull.at[j, pl.ds(aligned(c, half), half), :], loc.at[j]
        )
        for j in range(3)
    ]
    lat_local = pltpu.make_async_copy(latent, lat.at[z], loc.at[3])
    pos_local = pltpu.make_async_copy(pos_in, pos.at[z], loc.at[4])
    txt_local = pltpu.make_async_copy(text_kv.at[0, :, :, cols_of(c)], txt.at[c, z], loc.at[5])
    len_local = pltpu.make_async_copy(lens_in, lens.at[c], loc.at[6])
    out_local = pltpu.make_async_copy(w_out, wout, loc.at[7])
    my_piece = pl.ds(pl.multiple_of((c * ten_n + x) * piece, piece), piece)

    def copy_a(i):
        return remote(
            latent.at[my_piece], lat.at[z, my_piece], send_a.at[i], recv_a.at[z], seq=order(i)
        )

    def arrived_a(o):
        return remote(
            latent.at[my_piece], lat.at[o, my_piece], send_a.at[0], recv_a.at[o], seq=order(1)
        )

    def copy_b(o, t):
        to = (x + t) % ten_n
        return remote(
            lat.at[o, my_piece], lat.at[o, my_piece], send_b.at[o, t], recv_b.at[o, t], tensor=to
        )

    def arrived_b(o, t):
        source = (x + ten_n - t) % ten_n
        landed = pl.ds(pl.multiple_of((c * ten_n + source) * piece, piece), piece)
        return remote(
            lat.at[o, landed], lat.at[o, landed], send_b.at[o, t], recv_b.at[o, t], tensor=source
        )

    def copy_c(o, core):
        at = pl.ds(aligned(core, half_rows), half_rows)
        return remote(lat.at[o, at], lat.at[o, at], send_c.at[o], recv_c.at[o], cfg=other)

    def copy_p(i):
        return remote(pos_in, pos.at[z], send_p.at[i], recv_p.at[z], seq=order(i))

    def arrived_p(o):
        return remote(pos_in, pos.at[o], send_p.at[0], recv_p.at[o], seq=order(1))

    def copy_t(i, core):
        return remote(
            text_kv.at[0, :, :, cols_of(core)],
            txt.at[c, z],
            send_t.at[core, i],
            recv_t.at[c, z],
            seq=order(i),
            cfg=core,
        )

    def copy_t_mirror():
        return remote(
            text_kv.at[0, :, :, cols_of(other)],
            txt.at[c, z],
            send_t.at[other, 0],
            recv_t.at[c, z],
            cfg=other,
        )

    def arrived_t(core, o):
        return remote(
            text_kv.at[0, :, :, cols_of(c)], txt.at[core, o], send_t.at[c, 0], recv_t.at[core, o], cfg=other
        )

    def copy_l(core):
        return remote(lens_in, lens.at[core], send_l.at[0], recv_l.at[0], cfg=other)

    for j in range(3):
        w_local[j].start()
    lat_local.start()
    pos_local.start()
    txt_local.start()
    len_local.start()
    out_local.start()

    barrier = pltpu.get_barrier_semaphore()
    pl.semaphore_signal(barrier, inc=1, device_id={"cfg": other}, device_id_type=MESH)
    for t in range(1, ten_n):
        pl.semaphore_signal(
            barrier, inc=1, device_id={"tensor": (x + t) % ten_n}, device_id_type=MESH
        )
    for s in range(1, seq_n):
        for k in range(2):
            pl.semaphore_signal(
                barrier,
                inc=1,
                device_id={"seq": (z + s) % seq_n, "cfg": (c + k) % 2},
                device_id_type=MESH,
            )
    pl.semaphore_wait(barrier, 1 + (ten_n - 1) + 2 * (seq_n - 1))

    for j in range(3):
        w_copy[j].start()

    @pl.loop(1, seq_n)
    def _(i):
        copy_p(i).start()
        copy_a(i).start()

    copy_l(c).start()
    copy_t_mirror().start()

    @pl.loop(1, seq_n)
    def _(i):
        copy_t(i, 0).start()
        copy_t(i, 1).start()

    acc[...] = jnp.zeros_like(acc)
    lsum[...] = jnp.zeros_like(lsum)
    lat_local.wait()
    pos_local.wait()

    def pump_a(i):
        o = order(i)
        arrived_a(o).wait_recv()
        for t in range(1, ten_n):
            copy_b(o, t).start()

    def pump_b(i):
        o = order(i)
        for t in range(1, ten_n):
            arrived_b(o, t).wait_recv()
        copy_c(o, c).start()

    def normed_head(value, gain):
        return (
            value * lax.rsqrt(jnp.mean(value * value, axis=-1, keepdims=True) + 1e-06) * gain
        )

    def turned(value):
        total = value * tab[0]
        for k, shift in enumerate(ROT_SHIFTS):
            total = total + pltpu.roll(value, shift, 1) * tab[1 + k]
        return total

    def project(j, t):
        at = pl.ds(pl.multiple_of(t * tile, tile), tile)
        return [
            jnp.dot(mod[b * rows : (b + 1) * rows, :], wfull[j, :, at], preferred_element_type=F32)
            for b in range(2)
        ]

    def head_tiles(j, gain_row, dest):
        @pl.loop(0, mine // tile, unroll=U_TILE)
        def _(t):
            y = project(j, t)
            gain = gains[gain_row : gain_row + 1, :]
            for hh in range(per_tile):
                for b in range(2):
                    part_in = y[b][:, hh * HEAD_DIM : (hh + 1) * HEAD_DIM]
                    dest[b * heads + t * per_tile + hh] = turned(normed_head(part_in, gain)).astype(
                        BF16
                    )

    def value_tiles():
        @pl.loop(0, mine // tile, unroll=U_TILE)
        def _(t):
            y = [value.astype(BF16) for value in project(2, t)]
            for hh in range(per_tile):
                for b in range(2):
                    vbuf[b * heads + t * per_tile + hh] = y[b][:, hh * HEAD_DIM : (hh + 1) * HEAD_DIM]

    strip = 16

    @pl.loop(0, seq_n)
    def _(i):
        o = order(i)

        @pl.when(i > 0)
        def _():
            arrived_p(o).wait_recv()
            copy_c(o, other).wait_recv()

        place = lax.dot_general(
            pos[o], pick[...], (((0,), (0,)), ((), ())), preferred_element_type=F32
        )
        angle = place * rot[0:1, :]
        sine = jnp.sin(angle)
        tab[0] = jnp.cos(angle)
        for k in range(len(ROT_SHIFTS)):
            tab[1 + k] = sine * rot[1 + k : 2 + k, :]

        @pl.loop(0, rows // strip, unroll=U_MOD)
        def _(r):
            at = pl.ds(pl.multiple_of(r * strip, strip), strip)
            value = lat[o, at, :].astype(F32)
            center = value - jnp.mean(value, axis=-1, keepdims=True)
            normed = center * lax.rsqrt(jnp.mean(center * center, axis=-1, keepdims=True) + 1e-06)
            for b in range(2):
                mod[pl.ds(pl.multiple_of(b * rows + r * strip, strip), strip), :] = (
                    normed * (1.0 + modulation[1, b : b + 1, :]) + modulation[0, b : b + 1, :]
                ).astype(BF16)

        @pl.when(i == 0)
        def _():
            w_local[0].wait()
            w_copy[0].wait_recv()
            head_tiles(0, 0, qbuf)
            w_local[1].wait()
            w_copy[1].wait_recv()
            if seq_n > 1:
                pump_a(1)

        head_tiles(1, 1, kbuf)

        @pl.when(i == 0)
        def _():
            w_local[2].wait()
            w_copy[2].wait_recv()

        value_tiles()

        @pl.when(i + 1 < seq_n)
        def _():
            pump_b(i + 1)

        @pl.loop(0, 2 * heads, unroll=U_ATT)
        def _(h):
            scores = lax.dot_general(
                qbuf[h], kbuf[h], (((1,), (1,)), ((), ())), preferred_element_type=F32
            )
            expo = jnp.exp(scores * scale)
            folded = expo[:, :HEAD_DIM]
            for k in range(1, rows // HEAD_DIM):
                folded = folded + expo[:, k * HEAD_DIM : (k + 1) * HEAD_DIM]
            lsum[h] += folded
            acc[h] += jnp.dot(expo.astype(BF16), vbuf[h], preferred_element_type=F32)

        @pl.when(i + 2 < seq_n)
        def _():
            pump_a(i + 2)

    txt_local.wait()
    len_local.wait()
    copy_l(other).wait_recv()
    arrived_t(other, z).wait_recv()

    @pl.loop(1, seq_n)
    def _(i):
        arrived_t(0, order(i)).wait_recv()
        arrived_t(1, order(i)).wait_recv()

    text_rows = txt.shape[3]
    count = seq_n * text_rows
    for b in range(2):
        valid = lax.broadcasted_iota(jnp.int32, (1, count), 1).astype(F32) < lens[b, 0:1, :]

        @pl.loop(0, heads, unroll=U_TEXT)
        def _(h):
            at = pl.ds(pl.multiple_of(h * HEAD_DIM, HEAD_DIM), HEAD_DIM)
            raw = txt[b, :, 0, :, at].reshape(count, HEAD_DIM).astype(F32)
            keys = normed_head(raw, gains[1:2, :]).astype(BF16)
            values = txt[b, :, 1, :, at].reshape(count, HEAD_DIM)
            n = b * heads + h
            scores = lax.dot_general(
                qbuf[n], keys, (((1,), (1,)), ((), ())), preferred_element_type=F32
            )
            expo = jnp.where(valid, jnp.exp(scores * scale), 0.0)
            total = jnp.sum(lsum[n], axis=-1, keepdims=True) + jnp.sum(
                expo, axis=-1, keepdims=True
            )
            mixed = acc[n] + jnp.dot(expo.astype(BF16), values, preferred_element_type=F32)
            attf[c, b, :, at] = (mixed / total).astype(BF16)

    def copy_o(core):
        return remote(attf.at[core], attf.at[core], send_o.at[0], recv_o.at[0], cfg=other)

    copy_o(c).start()
    out_local.wait()
    copy_o(other).wait_recv()

    def copy_r(t):
        return remote(part.at[t], got.at[t], send_r.at[t], recv_r.at[t], tensor=(x + t) % ten_n)

    out_tile = 256 if out_cols % 256 == 0 else 128

    def out_block(t, k, at):
        to = (x + t) % ten_n
        here = pl.ds(pl.multiple_of(to * out_rows, out_rows), out_rows)
        total = None
        strength = guide[0:1, 0:1]
        at_gate = pl.ds(pl.multiple_of(c * out_cols + k * out_tile, out_tile), out_tile)
        gates = (
            strength * modulation[2, 0:1, at_gate],
            (1.0 - strength) * modulation[2, 1:2, at_gate],
        )
        for b in range(2):
            y = jnp.dot(attf[0, b, here, :], wout[0:mine, at], preferred_element_type=F32)
            y = y + jnp.dot(
                attf[1, b, here, :], wout[mine : 2 * mine, at], preferred_element_type=F32
            )
            y = y * gates[b]
            total = y if total is None else total + y
        return total

    for t in range(1, ten_n):

        @pl.loop(0, out_cols // out_tile)
        def _(k):
            at = pl.ds(pl.multiple_of(k * out_tile, out_tile), out_tile)
            part[t, :, at] = out_block(t, k, at).astype(BF16)

        copy_r(t).start()


    @pl.loop(0, out_cols // out_tile)
    def _(k):
        at = pl.ds(pl.multiple_of(k * out_tile, out_tile), out_tile)
        part[0, :, at] = out_block(0, k, at).astype(BF16)

    for t in range(1, ten_n):
        copy_r(t).wait_recv()
    total = part[0].astype(F32)
    for t in range(1, ten_n):
        total = total + got[t].astype(F32)
    out[...] = total.astype(BF16)

    for j in range(3):
        w_copy[j].wait_send()
    copy_l(c).wait_send()
    copy_t_mirror().wait_send()
    copy_o(c).wait_send()
    for t in range(1, ten_n):
        copy_r(t).wait_send()

    @pl.loop(1, seq_n)
    def _(i):
        copy_p(i).wait_send()
        copy_a(i).wait_send()
        copy_t(i, 0).wait_send()
        copy_t(i, 1).wait_send()
        o = order(i)
        for t in range(1, ten_n):
            copy_b(o, t).wait_send()
        copy_c(o, c).wait_send()


def local(
    seq_n, ten_n, latent, positions, text_kv, text_len, modulation, w_qkv, norm_gains, w_out, guidance
):
    rows, width = latent.shape
    mine = w_qkv.shape[2] // 2
    heads = mine // HEAD_DIM
    text_dev = text_kv.shape[2]
    out_rows = rows // ten_n
    out_cols = w_out.shape[1]
    pos_in = jnp.pad(positions.astype(BF16), ((0, 13), (0, 0)))
    lens = jnp.broadcast_to(text_len.astype(F32)[None, :], (8, seq_n * text_dev))
    any_space = pl.BlockSpec(memory_space=pl.ANY)
    vmem = pl.BlockSpec(memory_space=pltpu.VMEM)
    dma = pltpu.SemaphoreType.DMA
    return pl.pallas_call(
        functools.partial(kernel, seq_n, ten_n),
        out_shape=jax.ShapeDtypeStruct((out_rows, out_cols), BF16),
        in_specs=[
            any_space,
            any_space,
            any_space,
            any_space,
            vmem,
            any_space,
            vmem,
            any_space,
            vmem,
            vmem,
            vmem,
        ],
        out_specs=vmem,
        scratch_shapes=[
            pltpu.VMEM((seq_n, rows, width), BF16),
            pltpu.VMEM((seq_n, 16, rows), BF16),
            pltpu.VMEM((2, seq_n, 2, text_dev, mine), BF16),
            pltpu.VMEM((2, 8, seq_n * text_dev), F32),
            pltpu.VMEM((3, width, mine), BF16),
            pltpu.VMEM(w_out.shape, BF16),
            pltpu.VMEM((2 * rows, width), BF16),
            pltpu.VMEM((1 + len(ROT_SHIFTS), rows, HEAD_DIM), F32),
            pltpu.VMEM((2 * heads, rows, HEAD_DIM), BF16),
            pltpu.VMEM((2 * heads, rows, HEAD_DIM), BF16),
            pltpu.VMEM((2 * heads, rows, HEAD_DIM), BF16),
            pltpu.VMEM((2 * heads, rows, HEAD_DIM), F32),
            pltpu.VMEM((2 * heads, rows, HEAD_DIM), F32),
            pltpu.VMEM((2, 2, rows, mine), BF16),
            pltpu.VMEM((ten_n, out_rows, out_cols), BF16),
            pltpu.VMEM((ten_n, out_rows, out_cols), BF16),
            dma((seq_n,)),
            dma((seq_n,)),
            dma((seq_n, ten_n)),
            dma((seq_n, ten_n)),
            dma((seq_n,)),
            dma((seq_n,)),
            dma((seq_n,)),
            dma((seq_n,)),
            dma((2, seq_n)),
            dma((2, seq_n)),
            dma((3,)),
            dma((3,)),
            dma((1,)),
            dma((1,)),
            dma((1,)),
            dma((1,)),
            dma((ten_n,)),
            dma((ten_n,)),
            dma((8,)),
        ],
        compiler_params=pltpu.CompilerParams(
            collective_id=0, has_side_effects=True, vmem_limit_bytes=64 * 1024 * 1024 - 65536
        ),
    )(
        latent,
        pos_in,
        text_kv,
        lens,
        modulation,
        w_qkv,
        norm_gains,
        w_out,
        guidance.reshape(1, 1),
        jnp.asarray(ROT_ROWS),
        jnp.asarray(ROT_PICK, BF16),
    )


def solution(mesh):
    placed = (
        P(("groups", "seq"), None),
        P(None, ("groups", "seq")),
        P("cfg", None, ("groups", "seq"), "tensor"),
        P(("groups", "cfg")),
        P(None, "groups", None),
        P(None, "cfg", "tensor"),
        P(),
        P("tensor", "cfg"),
        P("groups"),
    )
    return jax.shard_map(
        functools.partial(local, mesh.shape["seq"], mesh.shape["tensor"]),
        mesh=mesh,
        in_specs=placed,
        out_specs=P(("groups", "seq", "tensor"), "cfg"),
        check_vma=False,
    )
```
